32 devices in a mesh: dp: 4 (over y, x), fsdp: 8 (over z, core).
Axes of the slice: x: 2, y: 2, z: 4, core: 2. Of those that a mesh axis runs over, the one named last changes fastest.
Arguments:
- inputs: bfloat16 [4, 16, 3584], P('dp', 'fsdp'), may hold values from -16 to 16
- baseline: bfloat16 [4, 16, 3584], P('dp', 'fsdp'), may hold values from -6 to 6
- cotangent: bfloat16 [4, 16, 3584], P('dp', 'fsdp'), may hold values from -6 to 6
- interval: int32 [4], P('dp'), may hold values from 0 to 7
- pre_gain: float32 [3584], replicated, may hold values from 0.1 to 1.9
- post_gain: float32 [3584], replicated, may hold values from 0.1 to 1.9
- gate_weight: bfloat16 [3584, 14336], P('dp', 'fsdp'), may hold values from -0.09375 to 0.09375
- up_weight: bfloat16 [3584, 14336], P('dp', 'fsdp'), may hold values from -0.09375 to 0.09375
- down_weight: bfloat16 [14336, 3584], P('fsdp', 'dp'), may hold values from -0.046875 to 0.046875
Outputs:
- attribution: float32 [4, 16, 3584], P('dp', 'fsdp')
The draws below stay inside these ranges and needn't reach their ends.
All inputs are finite; a program needn't handle non-finite values.
Results may differ from the reference program's by a relative error of at most 0.0027.
Values may be sent and summed in bfloat16 or wider, within the bound.
No kernel may reach another device: no remote copies, remote signals or barrier semaphores. Data moves between devices by JAX's collectives and lax.ppermute only.
A program may use at most 128 MiB of HBM per device.

```python
import math
import jax
import jax.numpy as jnp
from jax import lax

D = 3584
FF = 14336
STEPS = 4
SPANS = 8
TOTAL = 32
PROMPTS = 4
SEQ = 16


def draw_inputs(key, part):
    key_rows, key_cols, key_vals = jax.random.split(key, 3)
    rows_scale = jnp.exp(jax.random.uniform(key_rows, (PROMPTS, SEQ, 1), jnp.float32, math.log(0.3), math.log(3.0)))
    cols_scale = jnp.exp(jax.random.uniform(key_cols, (1, 1, D), jnp.float32, math.log(0.4), math.log(2.5)))
    values = jax.random.normal(key_vals, (PROMPTS, SEQ, D), jnp.float32) * rows_scale * cols_scale
    return jnp.clip(values, -16.0, 16.0).astype(jnp.bfloat16)


def touch_ends(values, rng, smallest, top_value):
    index_at = [jax.random.randint(jax.random.fold_in(rng, axis), (), 0, length) for axis, length in enumerate(values.shape)]
    main_axis = values.shape.index(max(values.shape))
    neighbour = index_at[:main_axis] + [(index_at[main_axis] + 1) % values.shape[main_axis]] + index_at[main_axis + 1:]
    return values.at[tuple(index_at)].set(smallest).at[tuple(neighbour)].set(top_value)


def block_scale(own_key, extent, cuts, low, high):
    level, own = 1.0, jax.random.fold_in(own_key, 6)
    for position, shards_of in cuts:
        heights = jnp.exp(jax.random.uniform(jax.random.fold_in(own, position), (shards_of,), jnp.float32, low / len(cuts), high / len(cuts)))
        level = level * jnp.repeat(heights, extent[position] // shards_of).reshape([-1 if axis == position else 1 for axis in range(len(extent))])
    return level


def scatter_about(rng, extent, scale, most, cuts=(), dtype=jnp.bfloat16):
    result = jax.random.normal(rng, extent, jnp.float32) * scale
    if len(cuts) > 0:
        result = block_scale(rng, extent, cuts, -0.22, 0.18) * result
    return jnp.clip(result, min=-most, max=most).astype(dtype)


def setup_inputs(seed: int = 0) -> dict:
    arg_keys = jax.random.split(jax.random.key(seed), 10)
    inputs = draw_inputs(jax.random.fold_in(arg_keys[9], 71), 0)
    baseline = scatter_about(arg_keys[1], (PROMPTS, SEQ, D), 1.0, 6.0, ((0, 4), (1, 8)))
    cotangent = scatter_about(arg_keys[2], (PROMPTS, SEQ, D), 1.0, 6.0, ((0, 4), (1, 8)))
    interval = touch_ends(jax.random.randint(arg_keys[3], (PROMPTS,), 0, SPANS), jax.random.fold_in(arg_keys[3], 1), 0, SPANS - 1).astype(jnp.int32)
    pre_gain = jnp.clip(1.0 + 0.18 * jax.random.normal(arg_keys[4], (D,), jnp.float32), 0.1, 1.9)
    post_gain = jnp.clip(1.0 + 0.18 * jax.random.normal(arg_keys[5], (D,), jnp.float32), 0.1, 1.9)
    gate_weight = scatter_about(arg_keys[6], (D, FF), D ** -0.5, 0.09375, ((0, 4), (1, 8)))
    up_weight = scatter_about(arg_keys[7], (D, FF), D ** -0.5, 0.09375, ((0, 4), (1, 8)))
    down_weight = scatter_about(arg_keys[8], (FF, D), FF ** -0.5, 0.046875, ((0, 8), (1, 4)))
    return dict(inputs=inputs, baseline=baseline, cotangent=cotangent, interval=interval, pre_gain=pre_gain, post_gain=post_gain, gate_weight=gate_weight, up_weight=up_weight, down_weight=down_weight)


epsilon = 1e-06
root_coef = math.sqrt(2.0 / math.pi)

def gelu_parts(argument):
    tangent = jnp.tanh(root_coef * (argument + 0.044715 * argument * argument * argument))
    gelu_value = 0.5 * argument * (1.0 + tangent)
    gelu_slope = 0.5 * (1.0 + tangent) + 0.5 * argument * (1.0 - tangent * tangent) * root_coef * (1.0 + 3.0 * 0.044715 * argument * argument)
    return (gelu_value, gelu_slope)

def norm_back(grad_in, source, gain):
    scaled = grad_in * gain
    inverse = lax.rsqrt(lax.optimization_barrier(jnp.mean(source * source, axis=-1, keepdims=True)) + epsilon)
    inner_mean = lax.optimization_barrier(jnp.mean(scaled * source, axis=-1, keepdims=True))
    return inverse * (scaled - source * inverse * inverse * inner_mean)

def reference(inputs, baseline, cotangent, interval, pre_gain, post_gain, gate_weight, up_weight, down_weight):
    source = inputs.astype(jnp.float32)
    anchor = baseline.astype(jnp.float32)
    target = cotangent.astype(jnp.float32).reshape(-1, D)
    offset = source - anchor
    summed = jnp.zeros(source.shape, jnp.float32)
    starts = interval.astype(jnp.float32)[:, None, None]
    for step_index in range(STEPS):
        fraction = (starts * STEPS + (step_index + 0.5)) / TOTAL
        sample_point = anchor + fraction * offset
        inverse = lax.rsqrt(lax.optimization_barrier(jnp.mean(sample_point * sample_point, axis=-1, keepdims=True)) + epsilon)
        normed = (sample_point * inverse * pre_gain).astype(jnp.bfloat16).reshape(-1, D)
        gate_val = jnp.dot(normed, gate_weight, preferred_element_type=jnp.float32)
        up_val = jnp.dot(normed, up_weight, preferred_element_type=jnp.float32)
        gelu_value, gelu_slope = gelu_parts(gate_val)
        hidden = (gelu_value * up_val).astype(jnp.bfloat16)
        branch = jnp.dot(hidden, down_weight, preferred_element_type=jnp.float32)
        branch_grad = norm_back(target, branch, post_gain).astype(jnp.bfloat16)
        hidden_grad = jnp.dot(branch_grad, down_weight.T, preferred_element_type=jnp.float32)
        gate_grad = (hidden_grad * up_val * gelu_slope).astype(jnp.bfloat16)
        up_grad = (hidden_grad * gelu_value).astype(jnp.bfloat16)
        normed_grad = jnp.dot(gate_grad, gate_weight.T, preferred_element_type=jnp.float32) + jnp.dot(up_grad, up_weight.T, preferred_element_type=jnp.float32)
        summed = summed + norm_back(normed_grad.reshape(source.shape), sample_point, pre_gain)
    return offset * summed / STEPS
```

```python
import functools
import math

import jax
import jax.numpy as jnp
import numpy as np
from jax import lax
from jax.experimental import pallas as pl
from jax.experimental.pallas import tpu as pltpu
from jax.sharding import PartitionSpec as P

STEPS = 4
TOTAL = 32
EPS = 1e-06
ROOT = math.sqrt(2.0 / math.pi)
G_SCALE = 16.0
U_SCALE = 64.0
V_TOP = 16384.0


f32, bf16, f16 = jnp.float32, jnp.bfloat16, jnp.float16


def swap(x, axis, size, mask):
    return lax.ppermute(x, axis, [(i, i ^ mask) for i in range(size)])


def split(x):
    hi = x.astype(bf16)
    return hi, (x - hi.astype(f32)).astype(bf16)


def dot_nn(a, b):
    return lax.dot_general(a, b, (((1,), (0,)), ((), ())), preferred_element_type=f32)


def dot_nt(a, b):
    return lax.dot_general(a, b, (((1,), (1,)), ((), ())), preferred_element_type=f32)


def up_to(n, k):
    return -(-n // k) * k


def kernel_call(body, outs, scratch=(), limit=24 << 20):
    return pl.pallas_call(
        body,
        out_shape=outs,
        scratch_shapes=list(scratch),
        compiler_params=pltpu.CompilerParams(vmem_limit_bytes=limit),
    )


def shape(s, d):
    return jax.ShapeDtypeStruct(s, d)


def solution(mesh):
    nd, nf = mesh.shape["dp"], mesh.shape["fsdp"]
    nz = nf // 2

    def spots():
        t = lax.axis_index("fsdp")
        return t >> 1, t & 1

    def first_kernel(ff, dl, own, rows8, model):
        ft = nf * own
        pick = np.zeros((4 * ft, nf * rows8), np.float32)
        for n in range(nf):
            for a in range(own):
                for part in range(3):
                    pick[part * ft + n * own + a, n * rows8 + part * own + a] = 1
                pick[3 * ft + n * own + a, n * rows8 + 3 * own] = 1
        roots = np.zeros((ft, nf * rows8), np.float32)
        belongs = np.zeros((ft, 128), np.float32)
        fold = np.zeros((128, 128), np.float32)
        for lane in range(3 * own * STEPS):
            fold[lane, lane % STEPS] = 1
            for n in range(nf):
                belongs[n * own + lane // STEPS % own, lane] = 1
        for n in range(nf):
            roots[n * own : (n + 1) * own, n * rows8 + 3 * own + 1] = 1

        def body(x_ref, y_ref, pick_ref, roots_ref, mask_ref, fold_ref, pre_ref, post_ref, gw_ref, uw_ref, g_ref, r_ref, u_ref, xs, lhs):
            zt, ct = spots()
            half = nd * 2 * ft
            for n in range(nf):
                j, c = (n >> 1) ^ zt, (n & 1) ^ ct
                xs[n] = jnp.where(c == 0, x_ref[j].astype(f32), y_ref[j].astype(f32))
            for m in range(nd):
                rows = xs[:, m * rows8 : (m + 1) * rows8, :].reshape(nf * rows8, dl).astype(bf16)
                got = dot_nn(pick_ref[...], rows)
                anchor = got[ft : 2 * ft]
                offset = got[:ft] - anchor
                start = got[3 * ft :]
                u_ref[m] = got[2 * ft : 3 * ft] * post_ref[...][:1]
                for k in (0, STEPS - 1):
                    hi, lo = split((anchor + (start + k / TOTAL) * offset) * pre_ref[...][:1])
                    at = m * 2 * ft + (ft if k else 0)
                    lhs[at : at + ft, :] = hi
                    lhs[half + at : half + at + ft, :] = lo
                if m == 0:
                    got = dot_nn(roots_ref[...], rows[:, :128]) * mask_ref[...]
                    r_ref[...] = dot_nn(got.astype(bf16), fold_ref[...])
            for i, w_ref in enumerate((gw_ref, uw_ref)):
                r = dot_nn(lhs[...], w_ref[...])
                r = (r[:half] + r[half:]) * G_SCALE
                for m in range(nd):
                    g_ref[m, i] = r[m * 2 * ft : (m + 1) * 2 * ft]

        call = kernel_call(
            body,
            [shape((nd, 2, 2 * ft, ff), f32), shape((ft, 128), f32), shape((nd, ft, dl), f32)],
            [pltpu.VMEM((nf, nd * rows8, dl), f32), pltpu.VMEM((nd * 4 * ft, dl), bf16)],
        )
        tables = (jnp.asarray(pick, bf16), jnp.asarray(roots, bf16), jnp.asarray(belongs), jnp.asarray(fold, bf16))
        return lambda x, y, *rest: call(x, y, *tables, *rest)

    def roots_kernel(own, model, dl, rows8):
        def body(x_ref, start_ref, first_ref, o_ref):
            anchor = x_ref[own : 2 * own, :].astype(f32)
            offset = x_ref[:own, :].astype(f32) - anchor
            lane = lax.broadcasted_iota(jnp.int32, (1, 128), 1)
            line = jnp.zeros((1, 128), f32)
            for k in range(STEPS):
                point = anchor + (start_ref[0] + k / TOTAL) * offset
                root = lax.rsqrt(jnp.mean(point * point, axis=1, keepdims=True) + EPS)
                for piece in range(3):
                    head = root.astype(bf16).astype(f32)
                    for a in range(own):
                        line = jnp.where(lane == (piece * own + a) * STEPS + k, head[a : a + 1], line)
                    root = root - head
            row = lax.broadcasted_iota(jnp.int32, (rows8, 128), 0)
            o_ref[...] = first_ref[...]
            o_ref[:, :128] = jnp.where(row == 3 * own + 1, line, first_ref[:, :128].astype(f32)).astype(bf16)

        return pl.pallas_call(
            body,
            in_specs=[
                pl.BlockSpec(memory_space=pltpu.VMEM),
                pl.BlockSpec(memory_space=pltpu.SMEM),
                pl.BlockSpec(memory_space=pltpu.VMEM),
            ],
            out_shape=shape((rows8, dl), bf16),
            compiler_params=pltpu.CompilerParams(vmem_limit_bytes=4 << 20),
            cost_estimate=pl.CostEstimate(flops=1 << 34, transcendentals=0, bytes_accessed=1 << 24),
        )

    def target_kernel(ff, dl, ft):
        def body(u_ref, dw_ref, o_ref):
            hi, lo = split(u_ref[...].reshape(nd * ft, dl))
            r = dot_nt(jnp.concatenate([hi, lo], 0), dw_ref[...])
            o_ref[...] = ((r[: nd * ft] + r[nd * ft :]) * U_SCALE).reshape(nd, ft, ff)

        return kernel_call(body, [shape((nd, ft, ff), f32)])

    def down_kernel(ff, dl, ft):
        rows = STEPS * ft
        block = nd * rows // nf

        def body(*refs):
            hs, (dw_ref, keep_ref, send_ref, lhs, res) = refs[:nd], refs[nd:]
            zt, ct = spots()
            for m in range(nd):
                lhs[m * rows : (m + 1) * rows, :] = hs[m][...]
            res[...] = dot_nn(lhs[...], dw_ref[...]).reshape(nf, block, dl)
            for j in range(nz):
                keep_ref[j] = res[((zt ^ j) << 1) | ct]
                send_ref[j] = res[((zt ^ j) << 1) | (ct ^ 1)].astype(bf16)

        return kernel_call(
            body,
            [shape((nz, block, dl), f32), shape((nz, block, dl), bf16)],
            [pltpu.VMEM((nd * rows, ff), bf16), pltpu.VMEM((nf, block, dl), f32)],
        )

    def back_kernel(ff, dl, ft):
        rows = STEPS * ft
        block = nd * rows // nf

        def body(*refs):
            x_ref, y_ref, u_ref, dw_ref = refs[:4]
            outs, lhs = refs[4 : 4 + nd], refs[4 + nd]
            zt, ct = spots()
            for b in range(nf):
                j, c = (b >> 1) ^ zt, (b & 1) ^ ct
                lhs[b * block : (b + 1) * block, :] = jnp.where(c == 0, x_ref[j].astype(f32), y_ref[j].astype(f32)).astype(bf16)
            r = dot_nt(lhs[...], dw_ref[...])
            for m in range(nd):
                outs[m][:, :ff] = r[m * rows : (m + 1) * rows].astype(bf16)
            lane = lax.broadcasted_iota(jnp.int32, (ft, 128), 1)
            for m in range(nd):
                u = u_ref[m]
                for k in range(STEPS):
                    s = lhs[m * rows + k * ft : m * rows + (k + 1) * ft, :].astype(f32)
                    ss = jnp.sum(s * s, axis=1, keepdims=True)
                    us = jnp.sum(s * u, axis=1, keepdims=True)
                    parts = jnp.zeros((ft, 128), f32)
                    for i, value in enumerate((ss, us)):
                        for piece in range(3):
                            head = value.astype(bf16).astype(f32)
                            parts = jnp.where(lane == 3 * i + piece, head, parts)
                            value = value - head
                    outs[m][k * ft : (k + 1) * ft, up_to(ff, 128) :] = parts.astype(bf16)

        return kernel_call(
            body,
            [shape((rows, up_to(ff, 128) + 128), bf16)] * nd,
            [pltpu.VMEM((nd * rows, dl), bf16)],
        )

    def middle_kernel(ff, ft, model):
        rows = STEPS * ft
        wide = up_to(ff, 128)

        def body(*refs):
            backs, (target_ref, ends_ref, inv_ref, v_ref, inner_ref) = refs[:nd], refs[nd:]
            lane = lax.broadcasted_iota(jnp.int32, (ft, 128), 1)
            gate_sum = up_sum = None
            inner = jnp.zeros((ft, 128), f32)
            for k in range(STEPS):
                at = slice(k * ft, (k + 1) * ft)
                through = backs[0][at, :].astype(f32)
                for m in range(1, nd):
                    through = through + backs[m][at, :].astype(f32)
                parts = through[:, wide:]
                squares = jnp.sum(jnp.where(lane < 3, parts, 0.0), axis=1, keepdims=True)
                dots = jnp.sum(jnp.where((lane >= 3) & (lane < 6), parts, 0.0), axis=1, keepdims=True)
                outer = lax.rsqrt(squares / model + EPS)
                hidden_grad = outer * target_ref[...] - (outer * outer * outer * (dots / model)) * through[:, :ff]
                r = inv_ref[:, k : k + 1]
                a = k / (STEPS - 1)
                gate = r * ((1 - a) * ends_ref[0, :ft] + a * ends_ref[0, ft:])
                up = r * ((1 - a) * ends_ref[1, :ft] + a * ends_ref[1, ft:])
                tangent = jnp.tanh(ROOT * (gate + 0.044715 * gate * gate * gate))
                act = 0.5 * gate * (1.0 + tangent)
                slope = 0.5 * (1.0 + tangent) + 0.5 * gate * (1.0 - tangent * tangent) * ROOT * (1.0 + 3.0 * 0.044715 * gate * gate)
                gate_grad = hidden_grad * up * slope
                up_grad = hidden_grad * act
                gate_sum = r * gate_grad if k == 0 else gate_sum + r * gate_grad
                up_sum = r * up_grad if k == 0 else up_sum + r * up_grad
                dot = r * r * jnp.sum(gate_grad * gate + up_grad * up, axis=1, keepdims=True)
                inner = jnp.where(lane == k, dot, inner)
            inner_ref[...] = inner
            most = jnp.max(jnp.maximum(jnp.abs(gate_sum), jnp.abs(up_sum)), axis=1, keepdims=True)
            level = jnp.ceil(jnp.log2(jnp.maximum(most, 1e-30)))
            v_ref[:, wide:] = jnp.broadcast_to(jnp.concatenate([level, level], 0), (2 * ft, 128))
            scale = V_TOP * jnp.exp2(-level)
            v_ref[:ft, :ff] = gate_sum * scale
            v_ref[ft:, :ff] = up_sum * scale

        return kernel_call(body, [shape((2 * ft, wide + 128), f32), shape((ft, 128), f32)])

    def last_kernel(ff, dl, own):
        ft = nf * own
        n_all = nd * ft
        wide = up_to(dl, 128)
        order = np.zeros((n_all, n_all), np.float32)
        for n in range(nf):
            for m in range(nd):
                for a in range(own):
                    order[n * nd * own + m * own + a, m * ft + n * own + a] = 1

        def body(*refs):
            vs, (order_ref, b_ref, gw_ref, uw_ref, keep_ref, send_ref, res) = refs[:nd], refs[nd:]
            zt, ct = spots()
            total = None
            for i, w_ref in enumerate((gw_ref, uw_ref)):
                at = slice(i * ft, (i + 1) * ft)
                pairs = [
                    split(v_ref[at, :ff] * (jnp.exp2(v_ref[at, up_to(ff, 128) :][:, :1]) * (1.0 / V_TOP))) for v_ref in vs
                ]
                lhs = [jnp.concatenate([pair[h] for pair in pairs], 0) for h in range(2)]
                lhs = jnp.concatenate([dot_nn(order_ref[...], part).astype(bf16) for part in lhs], 0)
                r = dot_nt(lhs, w_ref[...])
                total = r if total is None else total + r
            res[...] = jnp.zeros_like(res)
            res[:, :, :dl] = (total[:n_all] + total[n_all:]).reshape(nf, nd * own, dl)
            dots = b_ref[...]
            for n in range(nf):
                res[n, :own, wide:] = dots[n * own : (n + 1) * own]
            for j in range(nz):
                keep_ref[j] = res[((zt ^ j) << 1) | ct]
                send_ref[j] = res[((zt ^ j) << 1) | (ct ^ 1)]

        call = kernel_call(
            body,
            [shape((nz, nd * own, wide + 128), f32)] * 2,
            [pltpu.VMEM((nf, nd * own, wide + 128), f32)],
        )
        return lambda vs, *rest: call(*vs, jnp.asarray(order, bf16), *rest)

    def per_device(inputs, baseline, cotangent, interval, pre_gain, post_gain, gw, uw, dw):
        own, model = inputs.shape[1:]
        dl, ff = gw.shape
        ft = nf * own
        p = lax.axis_index("dp")
        over_dp = functools.partial(swap, axis="dp", size=nd)
        over_fsdp = functools.partial(swap, axis="fsdp", size=nf)

        start = (interval[0].astype(f32) * STEPS + 0.5) / TOTAL
        rows8 = up_to(3 * own + 2, 8)
        own_anchor = baseline[0].astype(f32)
        own_offset = inputs[0].astype(f32) - own_anchor
        points = [own_anchor + (start + k / TOTAL) * own_offset for k in range(STEPS)]
        raw = jnp.concatenate(
            [inputs[0], baseline[0], cotangent[0], jnp.full((rows8 - 3 * own, model), start.astype(bf16))], 0
        )
        cut = [lax.dynamic_slice(raw, (0, (p ^ m) * dl), (rows8, dl)) for m in range(nd)]
        others = [over_dp(cut[m], mask=m) for m in range(1, nd)]
        first = roots_kernel(own, model, dl, rows8)(raw, start[None], cut[0])
        mine = jnp.concatenate([first] + others, 0)
        column = jnp.stack([mine] + [over_fsdp(mine, mask=2 * j) for j in range(1, nz)])
        partner = over_fsdp(column, mask=1)
        pre_cut = jnp.broadcast_to(lax.dynamic_slice(pre_gain, (p * dl,), (dl,)), (8, dl))
        post_cut = jnp.broadcast_to(lax.dynamic_slice(post_gain, (p * dl,), (dl,)), (8, dl))

        g, inverse, u = first_kernel(ff, dl, own, rows8, model)(column, partner, pre_cut, post_cut, gw, uw)
        g16 = g.astype(f16)
        ends = g[0]
        for m in range(1, nd):
            ends = ends + over_dp(g16[m], mask=m).astype(f32)
        ends = ends * (1.0 / G_SCALE)

        hu = target_kernel(ff, dl, ft)(u, dw)[0]
        hu16 = hu.astype(f16)
        target = hu[0]
        for m in range(1, nd):
            target = target + over_dp(hu16[m], mask=m).astype(f32)
        target = target * (1.0 / U_SCALE)

        hidden = []
        for k in range(STEPS):
            a, r = k / (STEPS - 1), inverse[:, k : k + 1]
            gate = r * ((1 - a) * ends[0, :ft] + a * ends[0, ft:])
            up = r * ((1 - a) * ends[1, :ft] + a * ends[1, ft:])
            act = 0.5 * gate * (1.0 + jnp.tanh(ROOT * (gate + 0.044715 * gate * gate * gate)))
            hidden.append((act * up).astype(bf16))
        hidden = jnp.concatenate(hidden, 0)
        slots = [hidden] + [over_dp(hidden, mask=m) for m in range(1, nd)]

        keep, send = down_kernel(ff, dl, ft)(*slots, dw)
        keep = keep + over_fsdp(send, mask=1).astype(f32)
        keep16 = keep.astype(bf16)
        branch = keep[0]
        for j in range(1, nz):
            branch = branch + over_fsdp(keep16[j], mask=2 * j).astype(f32)
        branch, target = lax.optimization_barrier((branch.astype(bf16), target))
        column = jnp.stack([branch] + [over_fsdp(branch, mask=2 * j) for j in range(1, nz)])
        partner = over_fsdp(column, mask=1)

        back = back_kernel(ff, dl, ft)(column, partner, u, dw)
        back = [back[0]] + [over_dp(back[m], mask=m) for m in range(1, nd)]
        both, inner = middle_kernel(ff, ft, model)(*back, target, ends, inverse)
        both16 = both.astype(f16)
        whole = [both] + [over_dp(both16, mask=m).astype(f32) for m in range(1, nd)]

        keep, send = last_kernel(ff, dl, own)(whole, inner, gw, uw)
        keep = keep + over_fsdp(send, mask=1)
        final = keep[0]
        for j in range(1, nz):
            final = final + over_fsdp(keep[j], mask=2 * j)
        wide = up_to(dl, 128)
        pieces = jnp.stack([final[m * own : (m + 1) * own, :dl] if m == 0 else over_dp(final[m * own : (m + 1) * own, :dl], mask=m) for m in range(nd)])
        grads = jnp.concatenate([lax.dynamic_index_in_dim(pieces, p ^ j, 0, keepdims=False) for j in range(nd)], 1)
        dots = final[:own, wide : wide + STEPS] / model
        total = pre_gain * grads
        for k in range(STEPS):
            total = total - points[k] * dots[:, k : k + 1]
        return (own_offset * total / STEPS)[None]

    return jax.shard_map(
        per_device,
        mesh=mesh,
        in_specs=(
            P("dp", "fsdp", None),
            P("dp", "fsdp", None),
            P("dp", "fsdp", None),
            P("dp"),
            P(),
            P(),
            P("dp", "fsdp"),
            P("dp", "fsdp"),
            P("fsdp", "dp"),
        ),
        out_specs=P("dp", "fsdp", None),
        check_vma=False,
    )
```
